8 devices in a mesh: batch: 1 (over z), stage: 2 (over y), seq: 4 (over x, core).
Axes of the slice: x: 2, y: 2, z: 1, core: 2. Of those that a mesh axis runs over, the one named last changes fastest.
Arguments:
- x_tokens: bfloat16 [2, 4096, 4096], P('batch', 'seq')
- norm_attn: bfloat16 [2, 4096], P('stage')
- w_query: bfloat16 [2, 4096, 4096], P('stage')
- w_key: bfloat16 [2, 4096, 4096], P('stage')
- w_value: bfloat16 [2, 4096, 8192], P('stage')
- w_gate: bfloat16 [2, 4096, 16], P('stage')
- gate_bias: float32 [2, 16], P('stage')
- norm_out: bfloat16 [2, 512], P('stage')
- w_out: bfloat16 [2, 8192, 4096], P('stage')
- norm_mlp: bfloat16 [2, 4096], P('stage')
- w_up: bfloat16 [2, 4096, 8192], P('stage')
- w_down: bfloat16 [2, 8192, 4096], P('stage')
Outputs:
- output 1: bfloat16 [2, 2, 4096, 4096], P('stage', 'batch', 'seq')
- output 2: float32 [2, 2, 16, 256, 512], P('stage', 'batch')
All inputs are finite; a program needn't handle non-finite values.
Results may differ from the reference program's by a relative error of at most 0.0132003.
Values are sent between devices in bfloat16 or wider.
A program may use at most 1.5 GiB of HBM per device.

```python
import math
import jax
import jax.numpy as jnp
from jax import lax

NUM_SEQS = 2
CHUNK_LEN = 1024
TOKENS = 4096
MODEL_DIM = 4096
NUM_HEADS = 16
KEY_DIM = 256
VAL_DIM = 512
FFN_DIM = 8192
LAYERS = 2
NORM_EPS = 1e-6
NUM_CHUNKS = TOKENS // CHUNK_LEN
TOTAL_ROWS = NUM_SEQS * TOKENS


def dense_weight(rng_key, fan_in, fan_out):
    raw_draw = jax.random.normal(rng_key, (LAYERS, fan_in, fan_out), jnp.float32)
    return (raw_draw * fan_in ** -0.5).astype(jnp.bfloat16)


def gain_vector(rng_key, vec_width):
    raw_draw = jax.random.normal(rng_key, (LAYERS, vec_width), jnp.float32)
    return (1.0 + 0.3 * raw_draw).astype(jnp.bfloat16)


def setup_inputs(seed: int = 0, part: int = 0) -> dict:
    base_key = jax.random.key(seed)
    token_keys = jax.random.split(jax.random.fold_in(base_key, part), 2)
    weight_keys = jax.random.split(base_key, 11)
    token_noise = jax.random.normal(token_keys[0], (NUM_SEQS, TOKENS, MODEL_DIM), jnp.float32)
    walk_steps = jax.random.normal(token_keys[1], (NUM_SEQS, TOKENS, MODEL_DIM), jnp.float32)
    token_drift = jnp.cumsum(walk_steps, axis=1) * TOKENS ** -0.5
    gate_bias = math.log(CHUNK_LEN) + jax.random.uniform(weight_keys[5], (LAYERS, NUM_HEADS), jnp.float32, 0.0, 1.5)
    return {
        'x_tokens': (token_noise + 0.7 * token_drift).astype(jnp.bfloat16),
        'norm_attn': gain_vector(weight_keys[0], MODEL_DIM),
        'w_query': dense_weight(weight_keys[1], MODEL_DIM, NUM_HEADS * KEY_DIM),
        'w_key': dense_weight(weight_keys[2], MODEL_DIM, NUM_HEADS * KEY_DIM),
        'w_value': dense_weight(weight_keys[3], MODEL_DIM, NUM_HEADS * VAL_DIM),
        'w_gate': dense_weight(weight_keys[4], MODEL_DIM, NUM_HEADS),
        'gate_bias': gate_bias,
        'norm_out': gain_vector(weight_keys[6], VAL_DIM),
        'w_out': dense_weight(weight_keys[7], NUM_HEADS * VAL_DIM, MODEL_DIM),
        'norm_mlp': gain_vector(weight_keys[8], MODEL_DIM),
        'w_up': dense_weight(weight_keys[9], MODEL_DIM, FFN_DIM),
        'w_down': dense_weight(weight_keys[10], FFN_DIM, MODEL_DIM),
    }


def rms_norm(values, gain_vec):
    mean_sq = jnp.mean(values * values, axis=-1, keepdims=True)
    return values * lax.rsqrt(mean_sq + NORM_EPS) * gain_vec.astype(jnp.float32)


def chunk_step(carry_state, chunk_in):
    q_blk, k_blk, v_blk, decay_blk = chunk_in
    cum_decay = jnp.cumsum(decay_blk, axis=1)
    total_decay = cum_decay[:, -1, :]
    q_f32 = q_blk.astype(jnp.float32)
    k_f32 = k_blk.astype(jnp.float32)
    v_f32 = v_blk.astype(jnp.float32)
    inter_out = jnp.einsum('schk,shkv->schv', q_f32, carry_state) * jnp.exp(cum_decay)[..., None]
    scores = jnp.einsum('schk,sjhk->shcj', q_f32, k_f32)
    cum_heads = jnp.swapaxes(cum_decay, 1, 2)
    causal = jnp.arange(CHUNK_LEN)[:, None] >= jnp.arange(CHUNK_LEN)[None, :]
    decay_mat = jnp.exp(jnp.where(causal, cum_heads[:, :, :, None] - cum_heads[:, :, None, :], -jnp.inf))
    intra_out = jnp.einsum('shcj,sjhv->schv', scores * decay_mat, v_f32)
    k_decayed = k_f32 * jnp.exp(total_decay[:, None, :] - cum_decay)[..., None]
    new_state = jnp.exp(total_decay)[:, :, None, None] * carry_state + jnp.einsum('sjhk,sjhv->shkv', k_decayed, v_f32)
    return new_state, inter_out + intra_out


def to_chunks(values):
    shaped = values.reshape((NUM_SEQS, NUM_CHUNKS, CHUNK_LEN) + values.shape[1:])
    return jnp.moveaxis(shaped, 1, 0)


def layer_step(h_in, params):
    norm_attn, w_query, w_key, w_value, w_gate, gate_bias, norm_out, w_out, norm_mlp, w_up, w_down = params
    h_f32 = h_in.astype(jnp.float32).reshape(TOTAL_ROWS, MODEL_DIM)
    u_norm = rms_norm(h_f32, norm_attn).astype(jnp.bfloat16)
    q_all = jnp.dot(u_norm, w_query, preferred_element_type=jnp.float32).astype(jnp.bfloat16)
    k_all = (jnp.dot(u_norm, w_key, preferred_element_type=jnp.float32) * KEY_DIM ** -0.5).astype(jnp.bfloat16)
    v_all = jnp.dot(u_norm, w_value, preferred_element_type=jnp.float32).astype(jnp.bfloat16)
    log_decay = jax.nn.log_sigmoid(jnp.dot(u_norm, w_gate, preferred_element_type=jnp.float32) + gate_bias)
    chunks_in = (
        to_chunks(q_all.reshape(TOTAL_ROWS, NUM_HEADS, KEY_DIM)),
        to_chunks(k_all.reshape(TOTAL_ROWS, NUM_HEADS, KEY_DIM)),
        to_chunks(v_all.reshape(TOTAL_ROWS, NUM_HEADS, VAL_DIM)),
        to_chunks(log_decay),
    )
    zero_state = jnp.zeros((NUM_SEQS, NUM_HEADS, KEY_DIM, VAL_DIM), jnp.float32)
    final_state, chunk_outs = lax.scan(chunk_step, zero_state, chunks_in)
    attn_out = jnp.moveaxis(chunk_outs, 0, 1).reshape(TOTAL_ROWS, NUM_HEADS, VAL_DIM)
    head_norm = rms_norm(attn_out, norm_out).astype(jnp.bfloat16).reshape(TOTAL_ROWS, NUM_HEADS * VAL_DIM)
    h_mid = h_f32 + jnp.dot(head_norm, w_out, preferred_element_type=jnp.float32)
    mlp_in = rms_norm(h_mid, norm_mlp).astype(jnp.bfloat16)
    hidden = jax.nn.gelu(jnp.dot(mlp_in, w_up, preferred_element_type=jnp.float32), approximate=True).astype(jnp.bfloat16)
    h_out = (h_mid + jnp.dot(hidden, w_down, preferred_element_type=jnp.float32)).astype(jnp.bfloat16)
    h_out = h_out.reshape(NUM_SEQS, TOKENS, MODEL_DIM)
    return h_out, (h_out, final_state)


def reference(x_tokens, norm_attn, w_query, w_key, w_value, w_gate, gate_bias, norm_out, w_out, norm_mlp, w_up, w_down):
    params = (norm_attn, w_query, w_key, w_value, w_gate, gate_bias, norm_out, w_out, norm_mlp, w_up, w_down)
    last_h, (y_layers, s_final) = lax.scan(layer_step, x_tokens, params)
    return y_layers, s_final
```

```python
import functools

import jax
import jax.numpy as jnp
from jax import lax
from jax.experimental import pallas as pl
from jax.experimental.pallas import tpu as pltpu
from jax.sharding import PartitionSpec as P

NORM_EPS = 1e-6
CHUNK = 256
ROW_BLOCKS = 2
HEAD_GROUPS = 2
HEADS_STEP = 2
TILE = 1024
SUB = 512
NORM_ROWS = 64
COST_SCALE = 16


def rms_norm(values, gain_vec):
    mean_sq = jnp.mean(values * values, axis=-1, keepdims=True)
    return values * lax.rsqrt(mean_sq + NORM_EPS) * gain_vec.astype(jnp.float32)


def dot_f32(lhs, rhs):
    return jnp.dot(lhs, rhs, preferred_element_type=jnp.float32)


def head_column(cum_ref, head):
    cum = cum_ref[...]
    lane = lax.broadcasted_iota(jnp.int32, cum.shape, 1)
    return jnp.sum(jnp.where(lane == head, cum, 0.0), axis=1, keepdims=True)


def contract_rows(lhs, rhs):
    return lax.dot_general(lhs, rhs, (((0,), (0,)), ((), ())), preferred_element_type=jnp.float32)


def state_kernel(first_head, cum_ref, *refs):
    k_refs, v_refs, out_ref = refs[:ROW_BLOCKS], refs[ROW_BLOCKS:2 * ROW_BLOCKS], refs[-1]
    rows = k_refs[0].shape[0]
    key_dim, val_dim = out_ref.shape[1:]
    for sub in range(HEADS_STEP):
        head = first_head + HEADS_STEP * pl.program_id(0) + sub
        k_win, v_win = slice(sub * key_dim, (sub + 1) * key_dim), slice(sub * val_dim, (sub + 1) * val_dim)
        col = head_column(cum_ref, head)
        weight = jnp.exp(col[-1:, :] - col)
        total = None
        for blk in range(ROW_BLOCKS):
            k_dec = (k_refs[blk][:, k_win].astype(jnp.float32) * weight[blk * rows:(blk + 1) * rows]).astype(jnp.bfloat16)
            part = contract_rows(k_dec, v_refs[blk][:, v_win])
            total = part if total is None else total + part
        out_ref[sub] = total


def head_spec(arr, first_head, heads, width, rows):
    off = first_head // HEADS_STEP if arr.shape[1] > heads * width else 0
    return pl.BlockSpec((rows, HEADS_STEP * width), lambda h: (0, off + h))


def local_state(first_head, heads, key_dim, val_dim, cum, k_blks, v_blks):
    rows = k_blks[0].shape[0]
    tok = rows * ROW_BLOCKS
    return pl.pallas_call(
        functools.partial(state_kernel, first_head),
        grid=(heads // HEADS_STEP,),
        in_specs=[pl.BlockSpec(cum.shape, lambda h: (0, 0))]
        + [head_spec(k, first_head, heads, key_dim, rows) for k in k_blks]
        + [head_spec(v, first_head, heads, val_dim, rows) for v in v_blks],
        out_specs=pl.BlockSpec((HEADS_STEP, key_dim, val_dim), lambda h: (h, 0, 0)),
        out_shape=jax.ShapeDtypeStruct((heads, key_dim, val_dim), jnp.float32),
        compiler_params=pltpu.CompilerParams(vmem_limit_bytes=40 * 2**20),
        cost_estimate=pl.CostEstimate(
            flops=2 * heads * tok * key_dim * val_dim // COST_SCALE,
            bytes_accessed=heads * (2 * tok * (key_dim + val_dim) + 4 * key_dim * val_dim),
            transcendentals=heads * tok),
        name="local_state",
    )(cum, *k_blks, *v_blks)


def attn_kernel(first_head, dprev_ref, keep_ref, cum_ref, cum_t_ref, go_ref, *refs):
    nb = ROW_BLOCKS
    q_refs, k_refs, v_refs = refs[:nb], refs[nb:2 * nb], refs[2 * nb:3 * nb]
    near_ref, cross_ref, far_ref = refs[3 * nb:3 * nb + 3]
    o_refs, s_ref = refs[3 * nb + 3:4 * nb + 3], refs[4 * nb + 3]
    rows = q_refs[0].shape[0]
    key_dim, val_dim = s_ref.shape[1:]
    subs = range(HEADS_STEP)
    heads = [first_head + HEADS_STEP * pl.program_id(0) + sub for sub in subs]
    cols = [head_column(cum_ref, head) for head in heads]
    gain = go_ref[...].astype(jnp.float32)
    states = [near_ref[sub] + cross_ref[sub] + dprev_ref[heads[sub]] * far_ref[sub] for sub in subs]
    starts = [jnp.zeros((1, 1), jnp.float32) for _ in subs]
    causal = (lax.broadcasted_iota(jnp.int32, (CHUNK, CHUNK), 0)
              >= lax.broadcasted_iota(jnp.int32, (CHUNK, CHUNK), 1))
    for blk in range(nb):
        for part in range(rows // CHUNK):
            lo = blk * rows + part * CHUNK
            win = slice(part * CHUNK, (part + 1) * CHUNK)
            for sub in subs:
                k_win, v_win = slice(sub * key_dim, (sub + 1) * key_dim), slice(sub * val_dim, (sub + 1) * val_dim)
                state, start = states[sub], starts[sub]
                q, k, v = q_refs[blk][win, k_win], k_refs[blk][win, k_win], v_refs[blk][win, v_win]
                c_col = cols[sub][lo:lo + CHUNK]
                c_row = cum_t_ref[pl.ds(heads[sub], 1), lo:lo + CHUNK]
                end = c_col[-1:, :]
                scores = lax.dot_general(q, k, (((1,), (1,)), ((), ())), preferred_element_type=jnp.float32)
                decay = jnp.exp(jnp.where(causal, c_col - c_row, -jnp.inf))
                probs = (scores * decay).astype(jnp.bfloat16)
                out = dot_f32(q, state.astype(jnp.bfloat16)) * jnp.exp(c_col - start) + dot_f32(probs, v)
                mean_sq = jnp.mean(out * out, axis=1, keepdims=True)
                o_refs[blk][win, v_win] = (out * lax.rsqrt(mean_sq + NORM_EPS) * gain).astype(jnp.bfloat16)
                k_dec = (k.astype(jnp.float32) * jnp.exp(end - c_col)).astype(jnp.bfloat16)
                states[sub] = jnp.exp(end - start) * state + contract_rows(k_dec, v)
                starts[sub] = end
    for sub in subs:
        s_ref[sub] = jnp.where(keep_ref[0] > 0, states[sub], 0.0)


def attention(first_head, heads, key_dim, val_dim, dprev, keep, cum, cum_t, go, q_blks, k_blks, v_blks, near, cross, far):
    rows = q_blks[0].shape[0]
    tok = rows * ROW_BLOCKS
    spec = functools.partial(head_spec, first_head=first_head, heads=heads, rows=rows)
    st_spec = pl.BlockSpec((HEADS_STEP, key_dim, val_dim), lambda h: (h, 0, 0))
    n_chunks = tok // CHUNK
    outs = pl.pallas_call(
        functools.partial(attn_kernel, first_head),
        grid=(heads // HEADS_STEP,),
        in_specs=[pl.BlockSpec(memory_space=pltpu.SMEM),
                  pl.BlockSpec(memory_space=pltpu.SMEM),
                  pl.BlockSpec(cum.shape, lambda h: (0, 0)),
                  pl.BlockSpec(cum_t.shape, lambda h: (0, 0)),
                  pl.BlockSpec(go.shape, lambda h: (0, 0))]
        + [spec(q, width=key_dim) for q in q_blks] + [spec(k, width=key_dim) for k in k_blks]
        + [spec(v, width=val_dim) for v in v_blks] + [st_spec] * 3,
        out_specs=[pl.BlockSpec((rows, HEADS_STEP * val_dim), lambda h: (0, h))] * ROW_BLOCKS + [st_spec],
        out_shape=[jax.ShapeDtypeStruct((rows, heads * val_dim), jnp.bfloat16)] * ROW_BLOCKS
        + [jax.ShapeDtypeStruct((heads, key_dim, val_dim), jnp.float32)],
        compiler_params=pltpu.CompilerParams(vmem_limit_bytes=56 * 2**20),
        cost_estimate=pl.CostEstimate(
            flops=heads * n_chunks * CHUNK * (2 * key_dim * val_dim + CHUNK * (key_dim + val_dim)) // COST_SCALE,
            bytes_accessed=heads * (4 * tok * (key_dim + val_dim) + 16 * key_dim * val_dim),
            transcendentals=heads * tok * CHUNK),
        name="chunk_attention",
    )(dprev, keep, cum, cum_t, go, *q_blks, *k_blks, *v_blks, near, cross, far)
    return outs[:ROW_BLOCKS], outs[ROW_BLOCKS]


def pick_copies(flag_ref, sources, dst, sem):
    x_hbm, first_row, recv_hbm = sources
    from_x = pltpu.make_async_copy(x_hbm.at[pl.ds(first_row, dst.shape[0])], dst, sem)
    if recv_hbm is None:
        return from_x.start, from_x.wait
    from_recv = pltpu.make_async_copy(recv_hbm, dst, sem)

    def start():
        pl.when(flag_ref[0] == 0)(from_x.start)
        pl.when(flag_ref[0] != 0)(from_recv.start)

    return start, from_x.wait


def proj_kernel(jobs, first_row, with_recv, *refs):
    n_jobs = len(jobs)
    fused = first_row is not None
    refs = list(refs)
    take = refs.pop
    if fused:
        flag_ref, gain_ref, wg_ref, beta_ref, x_hbm = (take(0) for _ in range(5))
        recv_hbm = take(0) if with_recv else None
    else:
        u_hbm = take(0)
    w_refs = [take(0) for _ in range(n_jobs)]
    out_refs = [take(0) for _ in range(n_jobs)]
    if fused:
        u_out, gate_ref = take(0), take(0)
    u_ref, w_buf, o_buf, u_sem, w_sem, o_sem = refs

    def fetch(job, tile, slot):
        cols = pl.ds(pl.multiple_of(jobs[job][0] + tile * TILE, TILE), TILE)
        return pltpu.make_async_copy(w_refs[job].at[:, cols], w_buf.at[slot], w_sem.at[slot])

    def put(job, tile, slot):
        cols = pl.ds(pl.multiple_of(tile * TILE, TILE), TILE)
        return pltpu.make_async_copy(o_buf.at[slot], out_refs[job].at[:, cols], o_sem.at[slot])

    if fused:
        start, wait = pick_copies(flag_ref, (x_hbm, first_row, recv_hbm), u_ref, u_sem.at[0])
        start()
        fetch(0, 0, 0).start()
        wait()

        def norm_rows(index, carry):
            win = pl.ds(pl.multiple_of(index * NORM_ROWS, NORM_ROWS), NORM_ROWS)
            u_ref[win, :] = rms_norm(u_ref[win, :].astype(jnp.float32), gain_ref[...]).astype(jnp.bfloat16)
            return carry

        lax.fori_loop(0, u_ref.shape[0] // NORM_ROWS, norm_rows, 0)
        u_save = pltpu.make_async_copy(u_ref, u_out, u_sem.at[1])
        u_save.start()
        gate_ref[...] = dot_f32(u_ref[...], wg_ref[...]) + beta_ref[...]
    else:
        u_copy = pltpu.make_async_copy(u_hbm, u_ref, u_sem.at[0])
        u_copy.start()
        fetch(0, 0, 0).start()
        u_copy.wait()
    for job, (first_col, tiles, scale) in enumerate(jobs):
        assert tiles % 2 == 0

        def step(tile, carry, job=job, tiles=tiles, scale=scale):
            slot = lax.rem(tile, 2)

            @pl.when(tile + 1 < tiles)
            def _():
                fetch(job, tile + 1, 1 - slot).start()

            if job + 1 < n_jobs:
                @pl.when(tile + 1 == tiles)
                def _():
                    fetch(job + 1, 0, 0).start()

            fetch(job, tile, slot).wait()
            if job > 0:
                @pl.when(tile < 2)
                def _():
                    put(job - 1, tile, slot).wait()

            @pl.when(tile >= 2)
            def _():
                put(job, tile - 2, slot).wait()

            for sub in range(TILE // SUB):
                cols = slice(sub * SUB, (sub + 1) * SUB)
                acc = dot_f32(u_ref[...], w_buf[slot, :, cols])
                if scale != 1.0:
                    acc = acc * scale
                o_buf[slot, :, cols] = acc.astype(jnp.bfloat16)
            put(job, tile, slot).start()
            return carry

        lax.fori_loop(0, tiles, step, 0)
    for slot in range(2):
        put(n_jobs - 1, slot, slot).wait()
    if fused:
        u_save.wait()


def project(source, jobs, norm=None):
    any_spec = pl.BlockSpec(memory_space=pl.ANY)
    vmem = pl.BlockSpec(memory_space=pltpu.VMEM)
    depth = jobs[0][0].shape[0]
    weights = [job[0] for job in jobs]
    if norm is None:
        rows, first_row, recv = source.shape[0], None, None
        args, specs = [source], [any_spec]
    else:
        x_rows, first_row, rows, recv = source
        flag, gain, w_gate, bias = norm
        args = [flag, gain[None, :], w_gate, bias[None, :], x_rows] + ([] if recv is None else [recv])
        specs = [pl.BlockSpec(memory_space=pltpu.SMEM), vmem, vmem, vmem] + [any_spec] * (len(args) - 4)
    cols = sum(job[2] for job in jobs)
    out_shape = [jax.ShapeDtypeStruct((rows, job[2]), jnp.bfloat16) for job in jobs]
    out_specs = [any_spec] * len(jobs)
    if norm is not None:
        out_shape += [jax.ShapeDtypeStruct((rows, depth), jnp.bfloat16),
                      jax.ShapeDtypeStruct((rows, w_gate.shape[1]), jnp.float32)]
        out_specs += [any_spec, vmem]
    return pl.pallas_call(
        functools.partial(proj_kernel, tuple((job[1], job[2] // TILE, job[3]) for job in jobs), first_row, recv is not None),
        in_specs=specs + [any_spec] * len(jobs),
        out_specs=out_specs,
        out_shape=out_shape,
        scratch_shapes=[
            pltpu.VMEM((rows, depth), jnp.bfloat16),
            pltpu.VMEM((2, depth, TILE), jnp.bfloat16),
            pltpu.VMEM((2, rows, TILE), jnp.bfloat16),
            pltpu.SemaphoreType.DMA((2,)),
            pltpu.SemaphoreType.DMA((2,)),
            pltpu.SemaphoreType.DMA((2,)),
        ],
        compiler_params=pltpu.CompilerParams(vmem_limit_bytes=60 * 2**20),
        cost_estimate=pl.CostEstimate(
            flops=2 * rows * depth * cols // COST_SCALE,
            bytes_accessed=2 * (depth * cols + rows * (depth + cols)), transcendentals=0),
        name="project",
    )(*args, *weights)


def mlp_kernel(first_row, with_recv, with_buf, send, save_row, save_stage, *refs):
    g_n = HEAD_GROUPS
    refs = list(refs)
    take = refs.pop
    flag_ref, gain_ref, x_hbm = take(0), take(0), take(0)
    recv_hbm = take(0) if with_recv else None
    hn_hbm = [take(0) for _ in range(g_n)]
    wo_hbm, w1_hbm, w2_hbm = take(0), take(0), take(0)
    if with_buf:
        take(0)
    buf_hbm = take(0)
    y_hbm = take(0) if send else None
    h_ref, wide_ref, mid_ref, in_ref, w_buf, h_sem, hn_sem, w_sem, y_sem = refs
    rows, dim = h_ref.shape
    inner, wide = w_buf.shape[1], wide_ref.shape[1]
    part = wide // g_n
    col_tiles = dim // SUB
    up_tiles = wide // (2 * SUB)
    assert inner == wide and inner == 2 * dim and col_tiles % 2 == 0 and up_tiles % 2 == 0

    def window(index, width):
        return pl.ds(pl.multiple_of(index * width, width), width)

    hn_copies = [pltpu.make_async_copy(hn_hbm[g], wide_ref.at[:, g * part:(g + 1) * part], hn_sem.at[g]) for g in range(g_n)]
    h_start, h_wait = pick_copies(flag_ref, (x_hbm, first_row, recv_hbm), h_ref, h_sem)

    def deep(w_hbm, tile, slot):
        return [pltpu.make_async_copy(w_hbm.at[:, window(tile, SUB)], w_buf.at[slot], w_sem.at[slot, 0])]

    def flat(w_hbm, tile, slot):
        return [pltpu.make_async_copy(w_hbm.at[:, window(2 * tile + s, SUB)], w_buf.at[slot, pl.ds(s * dim, dim)], w_sem.at[slot, s])
                for s in range(2)]

    def start(copies):
        for copy in copies:
            copy.start()

    def stream(tiles, fetch, w_hbm, following, compute):
        def step(tile, carry):
            slot = lax.rem(tile, 2)

            @pl.when(tile + 1 < tiles)
            def _():
                start(fetch(w_hbm, tile + 1, 1 - slot))

            if following is not None:
                @pl.when(tile + 1 == tiles)
                def _():
                    start(following[0](following[1], 0, 0))

            for copy in fetch(w_hbm, tile, slot):
                copy.wait()
            compute(tile, slot)
            return carry

        lax.fori_loop(0, tiles, step, 0)

    start(deep(wo_hbm, 0, 0))
    start(hn_copies)
    h_start()
    for copy in hn_copies:
        copy.wait()
    h_wait()

    def out_proj(tile, slot):
        cols = window(tile, SUB)
        acc = dot_f32(wide_ref[...], w_buf[slot])
        mid_ref[:, cols] = h_ref[:, cols].astype(jnp.float32) + acc

    stream(col_tiles, deep, wo_hbm, (flat, w1_hbm), out_proj)

    def norm_rows(index, carry):
        win = window(index, NORM_ROWS)
        in_ref[win, :] = rms_norm(mid_ref[win, :], gain_ref[...]).astype(jnp.bfloat16)
        return carry

    lax.fori_loop(0, rows // NORM_ROWS, norm_rows, 0)

    def up_proj(tile, slot):
        for s in range(2):
            acc = dot_f32(in_ref[...], w_buf[slot, s * dim:(s + 1) * dim])
            wide_ref[:, window(2 * tile + s, SUB)] = jax.nn.gelu(acc, approximate=True).astype(jnp.bfloat16)

    stream(up_tiles, flat, w1_hbm, (deep, w2_hbm), up_proj)

    def each_copy(tile, act):
        cols = window(tile, SUB)
        if send:
            act(pltpu.make_async_copy(h_ref.at[:, cols], y_hbm.at[:, cols], y_sem.at[0, tile]))
        save = pltpu.make_async_copy(h_ref.at[:, cols], buf_hbm.at[pl.ds(save_row, rows), cols], y_sem.at[1, tile])
        if save_stage is None:
            act(save)
        else:
            pl.when(flag_ref[0] == save_stage)(lambda: act(save))

    def down_proj(tile, slot):
        cols = window(tile, SUB)
        acc = dot_f32(wide_ref[...], w_buf[slot])
        h_ref[:, cols] = (mid_ref[:, cols] + acc).astype(jnp.bfloat16)
        each_copy(tile, lambda copy: copy.start())

    stream(col_tiles, deep, w2_hbm, None, down_proj)
    for tile in range(col_tiles):
        each_copy(tile, lambda copy: copy.wait())


def mlp_block(flag, source, hn_groups, w_out, w_up, w_down, norm_mlp, y_buf, send, save_row, save_stage):
    x_rows, first_row, rows, recv = source
    dim, wide = w_up.shape
    any_spec = pl.BlockSpec(memory_space=pl.ANY)
    args = [flag, norm_mlp[None, :], x_rows] + ([] if recv is None else [recv]) + list(hn_groups) + [w_out, w_up, w_down]
    aliases = {}
    if y_buf is not None:
        aliases = {len(args): 0}
        args.append(y_buf)
    outs = pl.pallas_call(
        functools.partial(mlp_kernel, first_row, recv is not None, y_buf is not None, send, save_row, save_stage),
        in_specs=[pl.BlockSpec(memory_space=pltpu.SMEM), pl.BlockSpec(memory_space=pltpu.VMEM)] + [any_spec] * (len(args) - 2),
        out_specs=[any_spec] * (1 + send),
        out_shape=[jax.ShapeDtypeStruct(x_rows.shape, jnp.bfloat16)] + [jax.ShapeDtypeStruct((rows, dim), jnp.bfloat16)] * send,
        input_output_aliases=aliases,
        scratch_shapes=[
            pltpu.VMEM((rows, dim), jnp.bfloat16),
            pltpu.VMEM((rows, wide), jnp.bfloat16),
            pltpu.VMEM((rows, dim), jnp.float32),
            pltpu.VMEM((rows, dim), jnp.bfloat16),
            pltpu.VMEM((2, wide, SUB), jnp.bfloat16),
            pltpu.SemaphoreType.DMA,
            pltpu.SemaphoreType.DMA((len(hn_groups),)),
            pltpu.SemaphoreType.DMA((2, 2)),
            pltpu.SemaphoreType.DMA((2, dim // SUB)),
        ],
        compiler_params=pltpu.CompilerParams(vmem_limit_bytes=60 * 2**20),
        cost_estimate=pl.CostEstimate(
            flops=6 * rows * dim * wide // COST_SCALE, bytes_accessed=6 * dim * wide + 8 * rows * wide, transcendentals=rows * wide),
        name="mlp_block",
    )(*args)
    return outs[0], (outs[1] if send else None)


def after(value, *earlier):
    return lax.optimization_barrier((value,) + earlier)[0]


def layer_slot(flag, keep, x_rows, seq_row, recv, params, y_buf, send, save_row, save_stage, s_other, spread):
    norm_attn, w_query, w_key, w_value, w_gate, gate_bias, norm_out, w_out, norm_mlp, w_up, w_down = params
    num_heads = gate_bias.shape[0]
    key_dim = w_query.shape[1] // num_heads
    val_dim = norm_out.shape[0]
    heads = num_heads // HEAD_GROUPS
    k_cols, v_cols = heads * key_dim, heads * val_dim
    k_scale = key_dim ** -0.5
    rows = x_rows.shape[0] // (2 * ROW_BLOCKS)
    norm = (flag, norm_attn, w_gate, gate_bias)

    def kv_jobs(g):
        return [(w_key, g * k_cols, k_cols, k_scale), (w_value, g * v_cols, v_cols, 1.0)]

    source0 = (x_rows, seq_row, rows, recv and recv[0])
    q_job = (w_query, 0, w_query.shape[1], 1.0)
    k0, v0, q0, _, gate0 = project(
        source0, [(w_key, 0, w_key.shape[1], k_scale), (w_value, 0, w_value.shape[1], 1.0), q_job], norm)
    if recv:
        x_late, recv1 = x_rows, after(recv[1], k0)
    else:
        x_late, recv1 = after(x_rows, k0), None
    source1 = (x_late, seq_row + rows, rows, recv1)
    k1a, v1a, u1, gate1 = project(source1, kv_jobs(0), norm)
    cum = jnp.cumsum(jax.nn.log_sigmoid(jnp.concatenate([gate0, gate1], axis=0)), axis=0)
    cum_t = cum.T
    decay = jnp.exp(cum[-1, :])
    dprev = lax.ppermute(decay, 'seq', [(2, 3)])

    def local_part(g, k1, v1):
        loc = local_state(g * heads, heads, key_dim, val_dim, cum, [k0, k1], [v0, v1])
        return loc, lax.ppermute(loc, 'seq', [(0, 1), (2, 3)])

    def pair_state(g, loc, near):
        return loc + decay[g * heads:(g + 1) * heads, None, None] * near

    loc_a, near_a = local_part(0, k1a, v1a)
    pair_a = pair_state(0, loc_a, near_a)
    cross_a = lax.ppermute(pair_a, 'seq', [(1, 2)])
    k1b, v1b = project(after(u1, pair_a, dprev), kv_jobs(1))
    loc_b, near_b = local_part(1, k1b, v1b)
    cross_a = after(cross_a, loc_b)
    far_a = lax.ppermute(cross_a, 'seq', [(2, 3)])
    pair_b = pair_state(1, loc_b, after(near_b, cross_a))
    cross_b = lax.ppermute(pair_b, 'seq', [(1, 2)])
    (q1,) = project(after(u1, pair_b), [q_job])
    go = norm_out[None, :]
    o_a, s_a = attention(0, heads, key_dim, val_dim, dprev, keep, cum, cum_t, go, [q0, q1], [k0, k1a], [v0, v1a],
                         near_a, cross_a, far_a)
    cross_b = after(cross_b, s_a)
    far_b = lax.ppermute(cross_b, 'seq', [(2, 3)])
    o_b, s_b = attention(heads, heads, key_dim, val_dim, dprev, keep, cum, cum_t, go, [q0, q1], [k0, k1b], [v0, v1b],
                         near_b, cross_b, far_b)

    states = [s_a, s_b]
    parts = []
    if s_other is not None:
        states = [jnp.where(flag[0] == 0, other, own) for other, own in zip(s_other, states)]
    hn = [o_a[0], o_b[0]]
    if spread:
        hops = [lax.ppermute(state, 'seq', [(3, 1)]) for state in states]
        sides = [lax.ppermute(state, 'seq', [(3, 2)]) for state in states]
        hn[0] = after(hn[0], *states)
    y_buf, y0 = mlp_block(flag, source0, hn, w_out, w_up, w_down, norm_mlp, y_buf, send, save_row, save_stage)
    hn_late = after(o_a[1], y_buf)
    if spread:
        hops = [after(hop, y_buf) for hop in hops]
        ends = [lax.ppermute(hop, 'seq', [(1, 0)]) for hop in hops]
        hn_late = after(hn_late, *hops)
    y_buf, y1 = mlp_block(flag, source1, [hn_late, o_b[1]], w_out, w_up, w_down, norm_mlp, y_buf, send, save_row + rows, save_stage)
    if spread:
        parts = [(state, hop, after(side, y_buf), after(end, y_buf))
                 for state, hop, side, end in zip(states, hops, sides, ends)]
    return y_buf, [y0, y1], states, parts


def solution(mesh):
    num_stages = mesh.shape['stage']
    num_shards = mesh.shape['seq']
    assert num_stages == 2 and num_shards == 4
    mat_spec = P('stage', None, None)
    vec_spec = P('stage', None)
    weight_specs = (vec_spec, mat_spec, mat_spec, mat_spec, mat_spec, vec_spec, vec_spec, mat_spec, vec_spec, mat_spec, mat_spec)

    def device_program(x_tokens, norm_attn, w_query, w_key, w_value, w_gate, gate_bias, norm_out, w_out, norm_mlp, w_up, w_down):
        stage_idx = lax.axis_index('stage')
        seq_idx = lax.axis_index('seq')
        stacked = (norm_attn, w_query, w_key, w_value, w_gate, gate_bias, norm_out, w_out, norm_mlp, w_up, w_down)
        params = tuple(weight[0] for weight in stacked)
        x_rows = x_tokens.reshape(-1, x_tokens.shape[2])
        tok = x_tokens.shape[1]
        flag = stage_idx.astype(jnp.int32)[None]
        keep = (seq_idx == num_shards - 1).astype(jnp.int32)[None]

        def advance(y_blks):
            return [lax.ppermute(y, 'stage', [(0, 1)]) for y in y_blks]

        y_buf, y0, s0, _ = layer_slot(flag, keep, x_rows, 0, None, params, None, True, 0, None, None, False)
        y_buf, y1, _, first = layer_slot(flag, keep, x_rows, tok, advance(y0), params, y_buf, True, 0, 1, s0, True)
        y_buf, _, _, second = layer_slot(flag, keep, x_rows, tok, advance(y1), params, y_buf, False, tok, None, None, True)
        s_out = jnp.concatenate([a + b + c + d for a, b, c, d in first + second], axis=0)
        s_out = s_out.reshape((2, -1) + s_out.shape[1:])
        y_out = y_buf.reshape(x_tokens.shape)
        return y_out[None], s_out[None]

    return jax.shard_map(
        device_program,
        mesh=mesh,
        in_specs=(P('batch', 'seq', None),) + weight_specs,
        out_specs=(P('stage', 'batch', 'seq', None), P('stage', 'batch', None, None, None)),
        check_vma=False,
    )
```
